128 devices in a mesh: dp: 4 (over z_hi, core), seq: 32 (over y, z_lo, x).
Axes of the slice: x: 4, y: 4, z: 4 (z_hi: 2, z_lo: 2; z = z_hi * 2 + z_lo), core: 2. Of those that a mesh axis runs over, the one named last changes fastest.
Arguments:
- spectrum: bfloat16 [40960, 128], P(('dp', 'seq')), parts along dimension 0, may hold values from -7 to 7
- valid_frames: int32 [4], P('dp'), parts along dimension 0, may hold values from 1280 to 5120
- inlet_weight: bfloat16 [3, 128, 1280], replicated, may hold values from -0.3125 to 0.3125
- inlet_bias: float32 [1280], replicated, may hold values from -3 to 3
- stride_weight: bfloat16 [3, 1280, 1280], replicated, may hold values from -0.09375 to 0.09375
- stride_bias: float32 [1280], replicated, may hold values from -3 to 3
- norm_gain: float32 [1280], replicated, may hold values from 0.1 to 1.9
- norm_bias: float32 [1280], replicated, may hold values from -3 to 3
- projection_weight: bfloat16 [1280, 3840], replicated, may hold values from -1.2018865 to 1.2018865
- query_value_bias: float32 [2, 1280], replicated, may hold values from -5 to 5
- out_weight: bfloat16 [1280, 1280], replicated, may hold values from -0.15625 to 0.15625
- out_bias: float32 [1280], replicated, may hold values from -3 to 3
Outputs:
- attended: bfloat16 [20480, 1280], P(('dp', 'seq')), parts along dimension 0
- encoded: bfloat16 [20480, 1280], P(('dp', 'seq')), parts along dimension 0
The draws below stay inside these ranges and needn't reach their ends.
There are 4 independent parts, one for each index of `dp`. The reference program is written for one: setup_inputs(seed, part) draws one part's arguments, and reference() takes and returns one part's arrays. A program takes and returns all parts, laid end to end along the dimension named above; an argument that names none is the same for every part. Nothing has to cross between parts.
Inputs may be any that keep to these rules, and one draw needn't show every extreme that they name: Frames from valid_frames[0] on are padding and are never used as keys.
All inputs are finite; a program needn't handle non-finite values.
Results may differ from the reference program's by a relative error of at most 0.033.
Values may be sent and summed in bfloat16 or wider, within the bound.
No kernel may reach another device: no remote copies, remote signals or barrier semaphores. Data moves between devices by JAX's collectives and lax.ppermute only.
A program may use at most 256 MiB of HBM per device.

```python
import math
import jax
import jax.numpy as jnp
from jax import lax

D = 1280
HEADS = 20
HEAD_DIM = 64
MELS = 128
FRAMES_DEV = 160
FRAMES = 5120
MEL_FRAMES = 10240
N_SEQ = 32


def draw_spectrum(key, part):
    first_key = jax.random.fold_in(key, 0)
    return jnp.clip(jax.random.normal(first_key, (MEL_FRAMES, MELS), jnp.float32), -6.0, 6.0).astype(jnp.bfloat16)


def draw_projection_weight(key, part):
    first_key, second_key, third_key = jax.random.split(key, 3)
    factor = D ** (-0.5)
    first_draw = jnp.clip(jax.random.normal(first_key, (D, D), jnp.float32), -6.0, 6.0) * factor
    second_draw = jnp.clip(jax.random.normal(second_key, (D, D), jnp.float32), -6.0, 6.0) * factor
    third_draw = jnp.clip(jax.random.normal(third_key, (D, D), jnp.float32), -6.0, 6.0) * factor
    return jnp.concatenate([2.0 * first_draw, second_draw, third_draw], axis=1).astype(jnp.bfloat16)


def bell_draw(own_key, dims, deviation, reach, kind=jnp.bfloat16):
    return jnp.clip(deviation * jax.random.normal(own_key, dims, jnp.float32), -reach, reach).astype(kind)


def setup_inputs(seed: int = 0, part: int = 0) -> dict:
    seeds = jax.random.split(jax.random.key(seed), 13)
    own_keys = jax.random.split(jax.random.fold_in(seeds[12], part), 13)
    spectrum = draw_spectrum(jax.random.fold_in(jax.random.fold_in(seeds[12], part), 71), part)
    valid_frames = jax.random.randint(own_keys[1], (1,), FRAMES // 4, FRAMES + 1).astype(jnp.int32)
    inlet_weight = bell_draw(seeds[2], (3, MELS, D), (3 * MELS) ** -0.5, 0.3125)
    inlet_bias = bell_draw(seeds[3], (D,), 0.5, 3.0, jnp.float32)
    stride_weight = bell_draw(seeds[4], (3, D, D), (3 * D) ** -0.5, 0.09375)
    stride_bias = bell_draw(seeds[5], (D,), 0.5, 3.0, jnp.float32)
    norm_gain = jnp.clip(1.0 + 0.18 * jax.random.normal(seeds[6], (D,), jnp.float32), 0.1, 1.9)
    norm_bias = bell_draw(seeds[7], (D,), 0.5, 3.0, jnp.float32)
    projection_weight = draw_projection_weight(jax.random.fold_in(seeds[12], 71), part)
    query_value_bias = bell_draw(seeds[9], (2, D), 1.0, 5.0, jnp.float32)
    out_weight = bell_draw(seeds[10], (D, D), D ** -0.5, 0.15625)
    out_bias = bell_draw(seeds[11], (D,), 0.5, 3.0, jnp.float32)
    return {"spectrum": spectrum, "valid_frames": valid_frames, "inlet_weight": inlet_weight, "inlet_bias": inlet_bias, "stride_weight": stride_weight, "stride_bias": stride_bias, "norm_gain": norm_gain, "norm_bias": norm_bias, "projection_weight": projection_weight, "query_value_bias": query_value_bias, "out_weight": out_weight, "out_bias": out_bias}


masked_score = -1e+30
norm_epsilon = 1e-05

def gelu_exact(inputs):
    return jax.nn.gelu(inputs, approximate=False)

def sinusoids(first_frame, frame_count, model_width):
    half_width = model_width // 2
    increment = math.log(10000.0) / (half_width - 1)
    inverse = jnp.exp(-increment * jnp.arange(half_width, dtype=jnp.float32))
    moments = (first_frame + jnp.arange(frame_count, dtype=jnp.int32)).astype(jnp.float32)
    angles = moments[:, None] * inverse[None, :]
    return jnp.concatenate([jnp.sin(angles), jnp.cos(angles)], axis=1)

def reference(spectrum, valid_frames, inlet_weight, inlet_bias, stride_weight, stride_bias, norm_gain, norm_bias, projection_weight, query_value_bias, out_weight, out_bias):
    padded = jnp.pad(spectrum, ((1, 1), (0, 0)))
    stacked = jnp.concatenate([padded[0:MEL_FRAMES], padded[1:MEL_FRAMES + 1], padded[2:MEL_FRAMES + 2]], axis=1)
    first_conv = gelu_exact(jnp.dot(stacked, inlet_weight.reshape(3 * MELS, D), preferred_element_type=jnp.float32) + inlet_bias).astype(jnp.bfloat16)
    framed = jnp.pad(first_conv, ((1, 1), (0, 0)))
    paired = framed[0:2 * FRAMES].reshape(FRAMES, 2, D)
    stacked_two = jnp.concatenate([paired[:, 0], paired[:, 1], framed[2::2][0:FRAMES]], axis=1)
    second_conv = gelu_exact(jnp.dot(stacked_two, stride_weight.reshape(3 * D, D), preferred_element_type=jnp.float32) + stride_bias)
    stem_out = (second_conv + sinusoids(0, FRAMES, D)).astype(jnp.bfloat16)
    widened = stem_out.astype(jnp.float32)
    centre = lax.optimization_barrier(jnp.mean(widened, axis=1, keepdims=True))
    spread = lax.optimization_barrier(jnp.mean((widened - centre) ** 2, axis=1, keepdims=True))
    normed = ((widened - centre) * lax.rsqrt(spread + norm_epsilon) * norm_gain + norm_bias).astype(jnp.bfloat16)
    projected = jnp.dot(normed, projection_weight, preferred_element_type=jnp.float32)
    queries = (projected[:, 0:D] + query_value_bias[0]).astype(jnp.bfloat16)
    key_rows = projected[:, D:2 * D].astype(jnp.bfloat16)
    values = (projected[:, 2 * D:3 * D] + query_value_bias[1]).astype(jnp.bfloat16)
    queries, key_rows, values = lax.optimization_barrier((queries, key_rows, values))
    key_heads = key_rows.astype(jnp.float32).reshape(FRAMES, HEADS, HEAD_DIM)
    value_heads = values.astype(jnp.float32).reshape(FRAMES, HEADS, HEAD_DIM)
    key_live = jnp.arange(FRAMES, dtype=jnp.int32) < valid_frames[0]
    scaling = HEAD_DIM ** (-0.5)

    def attend_block(query_block):
        query_heads = query_block.astype(jnp.float32).reshape(FRAMES_DEV, HEADS, HEAD_DIM)
        scores = jnp.einsum('qhd,khd->qhk', query_heads, key_heads) * scaling
        scores = jnp.where(key_live[None, None, :], scores, masked_score)
        highest = lax.optimization_barrier(jnp.max(scores, axis=2, keepdims=True))
        weights = jnp.where(key_live[None, None, :], jnp.exp(scores - highest), 0.0)
        denominator = lax.optimization_barrier(jnp.sum(weights, axis=2))
        rounded = lax.optimization_barrier(weights.astype(jnp.bfloat16)).astype(jnp.float32)
        numerator = jnp.einsum('qhk,khd->qhd', rounded, value_heads)
        return (numerator / denominator[:, :, None]).reshape(FRAMES_DEV, D).astype(jnp.bfloat16)
    mixed_rows = lax.map(attend_block, queries.reshape(N_SEQ, FRAMES_DEV, D)).reshape(FRAMES, D)
    output = jnp.dot(mixed_rows, out_weight, preferred_element_type=jnp.float32) + out_bias
    return (output.astype(jnp.bfloat16), (stem_out.astype(jnp.float32) + output).astype(jnp.bfloat16))
```

```python
import math

import jax
import jax.numpy as jnp
from jax import lax
from jax.experimental import pallas as pl
from jax.experimental.pallas import tpu as pltpu
from jax.sharding import PartitionSpec as P

HEAD_DIM = 64
LANES = 128
GROUP = 8
norm_epsilon = 1e-05


def sinusoids(first_frame, frame_count, model_width):
    half_width = model_width // 2
    increment = math.log(10000.0) / (half_width - 1)
    inverse = jnp.exp(-increment * jnp.arange(half_width, dtype=jnp.float32))
    moments = (first_frame + jnp.arange(frame_count, dtype=jnp.int32)).astype(jnp.float32)
    angles = moments[:, None] * inverse[None, :]
    return jnp.concatenate([jnp.sin(angles), jnp.cos(angles)], axis=1)


def gelu(v):
    return 0.5 * v * (1.0 + lax.erf(v * (2.0**-0.5)))


def window(whole, rolled, start):
    if start % LANES == 0:
        return whole[:, start : start + LANES]
    return rolled[:, start - 64 : start + 64]


def ab_start(g):
    return 320 * (g // 2) + 192 * (g % 2)


def s_start(g):
    return 320 * (g // 2) + 128


def low_lanes(rows):
    return lax.broadcasted_iota(jnp.int32, (rows, LANES), 1) < 64


W2_PARTS = 6


def stem_kernel(
    first_ref, lhs_ref, pos_ref, b1_ref, b2_ref, gain_ref, nbias_ref, vbias_ref,
    w1_hbm, w2_hbm, wp_hbm,
    kv_ref, normed_ref, stem_ref,
    w1, w2, wkv, odd, sems,
):
    frames, width = stem_ref.shape
    part = w2.shape[0] // W2_PARTS
    c1 = pltpu.make_async_copy(w1_hbm, w1, sems.at[0])
    c1.start()
    c2 = []
    for i in range(W2_PARTS):
        rows = pl.ds(i * part, part)
        c2.append(pltpu.make_async_copy(w2_hbm.at[rows], w2.at[rows], sems.at[1 + i]))
        c2[-1].start()
    c3 = []
    for i in range(2):
        c3.append(
            pltpu.make_async_copy(
                wp_hbm.at[:, pl.ds(width * (1 + i), width)],
                wkv.at[:, pl.ds(width * i, width)],
                sems.at[1 + W2_PARTS + i],
            )
        )
        c3[-1].start()
    c1.wait()
    pad = lhs_ref.shape[0] - frames
    first = gelu(jnp.dot(lhs_ref[...], w1[...], preferred_element_type=jnp.float32) + b1_ref[...])
    row = lax.broadcasted_iota(jnp.int32, (pad, width), 0)
    dead = jnp.logical_and(row == 0, first_ref[0] != 0)
    odd[...] = jnp.where(dead, 0.0, first[:pad])
    before = odd[0:frames, :].astype(jnp.bfloat16)
    after = odd[1 : frames + 1, :].astype(jnp.bfloat16)
    even = first[pad:].astype(jnp.bfloat16)
    total = None
    per = W2_PARTS // 3
    for tap, rows in enumerate((before, even, after)):
        for i in range(per):
            c2[tap * per + i].wait()
            term = jnp.dot(
                rows[:, i * part : (i + 1) * part],
                w2[(tap * per + i) * part : (tap * per + i + 1) * part, :],
                preferred_element_type=jnp.float32,
            )
            total = term if total is None else total + term
    second = gelu(total + b2_ref[...])
    stem = (second + pos_ref[...]).astype(jnp.bfloat16)
    stem_ref[...] = stem
    wide = stem.astype(jnp.float32)
    centred = wide - jnp.mean(wide, axis=1, keepdims=True)
    spread = jnp.mean(centred * centred, axis=1, keepdims=True)
    normed = (centred * lax.rsqrt(spread + norm_epsilon) * gain_ref[...] + nbias_ref[...]).astype(jnp.bfloat16)
    normed_ref[...] = normed
    c3[0].wait()
    keys = jnp.dot(normed, wkv[:, :width], preferred_element_type=jnp.float32)
    c3[1].wait()
    values = jnp.dot(normed, wkv[:, width:], preferred_element_type=jnp.float32) + vbias_ref[...]
    keys_r = pltpu.roll(keys, width - 64, 1)
    values_r = pltpu.roll(values, width - 64, 1)
    low = low_lanes(frames)
    for g in range(GROUP):
        kv_ref[g, 0:frames, :] = window(keys, keys_r, ab_start(g)).astype(jnp.bfloat16)
        kv_ref[g, frames : 2 * frames, :] = window(values, values_r, ab_start(g)).astype(jnp.bfloat16)
        shared = jnp.where(low, window(keys, keys_r, s_start(g)), window(values, values_r, s_start(g) - 64))
        kv_ref[g, 2 * frames : 3 * frames, :] = shared.astype(jnp.bfloat16)


def query_kernel(normed_ref, bias_ref, w_ref, q_ref):
    frames, width = normed_ref.shape
    half = frames // 2
    scale = HEAD_DIM**-0.5 * math.log2(math.e)
    q = (jnp.dot(normed_ref[...], w_ref[...], preferred_element_type=jnp.float32) + bias_ref[...]) * scale
    q_r = pltpu.roll(q, width - 64, 1)
    low = low_lanes(half)
    for g in range(GROUP):
        q_ref[g, 0:frames, :] = window(q, q_r, ab_start(g)).astype(jnp.bfloat16)
        rows = slice(half * (g % 2), half * (g % 2 + 1))
        shared = window(q, q_r, s_start(g))[rows]
        q_ref[g, frames : frames + half, :] = jnp.where(low, shared, 0.0).astype(jnp.bfloat16)


NEG = -1e30
STEP = 2


def attend_kernel(*refs, chunks, opening, closing):
    refs = list(refs)
    info = refs.pop(0)
    q_ref = refs.pop(0)
    kv_refs = [refs.pop(0) for _ in range(chunks)]
    if opening:
        old = None
    else:
        old = [refs.pop(0) for _ in range(3)]
    if closing:
        o_ref = refs.pop(0)
        state = [refs.pop(0) for _ in range(3)]
    else:
        state = [refs.pop(0) for _ in range(3)]
    k_ab, v_ab, k_s, v_s = refs
    m_ref, l_ref, a_ref = state
    span = k_ab.shape[0]
    frames = kv_refs[0].shape[1] // 3
    half = frames // 2
    if opening:
        m_ref[...] = jnp.full(m_ref.shape, NEG, jnp.float32)
        l_ref[...] = jnp.zeros(l_ref.shape, jnp.float32)
        a_ref[...] = jnp.zeros(a_ref.shape, jnp.float32)
    else:
        for new, was in zip(state, old):
            new[...] = was[...]

    def update(q, k, v, m_old):
        s = lax.dot_general(q, k, (((1,), (1,)), ((), ())), preferred_element_type=jnp.float32)
        m_new = jnp.maximum(m_old, jnp.max(s, axis=1, keepdims=True))
        p = jnp.exp2(s - m_new).astype(jnp.bfloat16)
        out = jnp.dot(p, v, preferred_element_type=jnp.float32)
        return m_new, out

    for c in range(chunks):
        live = info[0] - info[1 + c]

        @pl.when(live > 0)
        def _():
            kv = kv_refs[c]
            alive = lax.broadcasted_iota(jnp.int32, (span, LANES), 0) < live

            def put(ref, lanes, got):
                ref[:, lanes] = got.astype(jnp.bfloat16)

            ones = jnp.where(alive, 1.0, 0.0)
            kab = kv[:, 0:frames, :].reshape(span, LANES).astype(jnp.float32)
            vab = kv[:, frames : 2 * frames, :].reshape(span, LANES).astype(jnp.float32)
            sh = kv[:, 2 * frames : 3 * frames, :].reshape(span, LANES).astype(jnp.float32)
            put(k_ab, slice(0, LANES), jnp.where(alive, kab, kab[0:1]))
            put(v_ab, slice(0, LANES), jnp.where(alive, vab, 0.0))
            put(v_ab, slice(LANES, 2 * LANES), ones)
            put(k_s, slice(0, LANES), jnp.where(alive, sh, sh[0:1]))
            put(v_s, slice(0, LANES), jnp.where(alive, sh, 0.0))
            put(v_s, slice(LANES, 2 * LANES), ones)

            def step(i, carry):
                rows = STEP * frames
                at = pl.ds(pl.multiple_of(i * rows, rows), rows)
                q = q_ref[pl.ds(i * STEP, STEP), 0:frames, :].reshape(rows, LANES)
                low = low_lanes(rows)
                zero = jnp.zeros_like(q)
                qq = jnp.concatenate([jnp.where(low, q, zero), jnp.where(low, zero, q)], axis=0)
                m = m_ref[at, :]
                m_new, out = update(qq, k_ab[...], v_ab[...], jnp.concatenate([m[:, 0:1], m[:, 64:65]], axis=0))
                m_two = jnp.where(low, m_new[:rows], m_new[rows:])
                keep = jnp.exp2(m - m_two)
                m_ref[at, :] = m_two
                a_ref[at, :] = a_ref[at, :] * keep + jnp.where(low, out[:rows, :LANES], out[rows:, :LANES])
                l_ref[at, :] = l_ref[at, :] * keep + jnp.where(low, out[:rows, LANES:], out[rows:, LANES:])
                few = STEP * half
                at = pl.ds(pl.multiple_of(GROUP * frames + i * few, few), few)
                qs = q_ref[pl.ds(i * STEP, STEP), frames : frames + half, :].reshape(few, LANES)
                m = m_ref[at, :]
                m_new, out = update(qs, k_s[...], v_s[...], m[:, 0:1])
                m_two = jnp.broadcast_to(m_new, m.shape)
                keep = jnp.exp2(m - m_two)
                m_ref[at, :] = m_two
                a_ref[at, :] = a_ref[at, :] * keep + out[:, :LANES]
                l_ref[at, :] = l_ref[at, :] * keep + out[:, LANES:]
                return carry

            lax.fori_loop(0, GROUP // STEP, step, 0)

    if closing:
        cut = GROUP * frames
        o_ref[:, 0:frames, :] = (a_ref[0:cut, :] / l_ref[0:cut, :]).astype(jnp.bfloat16).reshape(GROUP, frames, LANES)
        rest = jnp.where(low_lanes(GROUP * half), 0.0, a_ref[cut:, :] / l_ref[cut:, :])
        o_ref[:, frames : frames + half, :] = rest.astype(jnp.bfloat16).reshape(GROUP, half, LANES)


def output_kernel(o_ref, w_ref, bias_ref, stem_ref, attended_ref, encoded_ref):
    frames, width = stem_ref.shape
    half = frames // 2
    total = None
    for g in range(GROUP):
        at = ab_start(g)
        term = jnp.dot(o_ref[g, 0:frames, :], w_ref[at : at + LANES, :], preferred_element_type=jnp.float32)
        total = term if total is None else total + term
        if g % 2:
            at = s_start(g) - 64
            shared = jnp.concatenate(
                [o_ref[g - 1, frames : frames + half, :], o_ref[g, frames : frames + half, :]], axis=0
            )
            total = total + jnp.dot(shared, w_ref[at : at + LANES, :], preferred_element_type=jnp.float32)
    total = total + bias_ref[...]
    attended_ref[...] = total.astype(jnp.bfloat16)
    encoded_ref[...] = (stem_ref[...].astype(jnp.float32) + total).astype(jnp.bfloat16)


VMEM = pltpu.MemorySpace.VMEM
SMEM = pltpu.MemorySpace.SMEM


def spec(space):
    return pl.BlockSpec(memory_space=space)


def params(mib):
    return pltpu.CompilerParams(vmem_limit_bytes=mib * 2**20)


def shards(
    spectrum, valid_frames, inlet_weight, inlet_bias, stride_weight, stride_bias, norm_gain, norm_bias,
    projection_weight, query_value_bias, out_weight, out_bias,
):
    mel_rows, channels = spectrum.shape
    frames = mel_rows // 2
    width = projection_weight.shape[0]
    count = lax.axis_size("seq")
    me = lax.axis_index("seq")
    pairs = spectrum.reshape(frames, 2 * channels)
    down = [(i, i + 1) for i in range(count - 1)]
    up = [(i + 1, i) for i in range(count - 1)]
    earlier = lax.ppermute(pairs[frames - 1 :], "seq", down)
    later = lax.ppermute(pairs[:1], "seq", up)
    wide = jnp.concatenate([earlier, pairs, later], axis=0)
    odd_rows = jnp.concatenate([wide[0 : frames + 1], wide[1 : frames + 2, :channels]], axis=1)
    even_rows = jnp.concatenate([wide[0:frames, channels:], wide[1 : frames + 1]], axis=1)
    pad = 16
    lhs = jnp.concatenate([jnp.pad(odd_rows, ((0, pad - 1), (0, 0))), even_rows], axis=0)
    position = sinusoids(me * frames, frames, width)
    first = (me == 0).astype(jnp.int32).reshape(1)
    row = lambda v: v.reshape(1, width)
    bf16 = lambda *dims: jax.ShapeDtypeStruct(dims, jnp.bfloat16)
    f32 = lambda *dims: jax.ShapeDtypeStruct(dims, jnp.float32)

    kv, normed, stem = pl.pallas_call(
        stem_kernel,
        name="stem",
        out_shape=(bf16(GROUP, 3 * frames, LANES), bf16(frames, width), bf16(frames, width)),
        in_specs=[spec(SMEM)] + [spec(VMEM)] * 7 + [spec(pltpu.MemorySpace.HBM)] * 3,
        out_specs=(spec(VMEM),) * 3,
        scratch_shapes=[
            pltpu.VMEM((3 * channels, width), jnp.bfloat16),
            pltpu.VMEM((3 * width, width), jnp.bfloat16),
            pltpu.VMEM((width, 2 * width), jnp.bfloat16),
            pltpu.VMEM((frames + pad, width), jnp.float32),
            pltpu.SemaphoreType.DMA((3 + W2_PARTS,)),
        ],
        compiler_params=params(40),
        cost_estimate=pl.CostEstimate(flops=4 * 10**9, bytes_accessed=20 * 10**6, transcendentals=0),
    )(
        first, lhs, position, row(inlet_bias), row(stride_bias), row(norm_gain), row(norm_bias),
        row(query_value_bias[1]),
        inlet_weight.reshape(3 * channels, width), stride_weight.reshape(3 * width, width), projection_weight,
    )

    teams = [list(range(i, i + GROUP)) for i in range(0, count, GROUP)]
    swap = lambda v: lax.all_to_all(v, "seq", 0, 0, axis_index_groups=teams)
    kv = swap(kv)
    spans = count // GROUP
    shift = lambda v, by: lax.ppermute(v, "seq", [(i, (i + by * GROUP) % count) for i in range(count)])
    others = [shift(kv, by) for by in (1, spans - 1, 2)]

    query = pl.pallas_call(
        query_kernel,
        name="query",
        grid=(1,),
        out_shape=bf16(GROUP, frames + frames // 2, LANES),
        in_specs=[
            pl.BlockSpec((frames, width), lambda i: (0, 0)),
            pl.BlockSpec((1, width), lambda i: (0, 0)),
            pl.BlockSpec((width, width), lambda i: (0, 0)),
        ],
        out_specs=pl.BlockSpec((GROUP, frames + frames // 2, LANES), lambda i: (0, 0, 0)),
        compiler_params=params(20),
        cost_estimate=pl.CostEstimate(flops=10**9, bytes_accessed=4 * 10**6, transcendentals=0),
    )(normed, row(query_value_bias[0]), projection_weight)
    query = swap(query)

    live = valid_frames[0]
    mine = me // GROUP
    span = GROUP * frames
    rows = span + span // 2
    scratch = [
        pltpu.VMEM((span, LANES), jnp.bfloat16),
        pltpu.VMEM((span, 2 * LANES), jnp.bfloat16),
        pltpu.VMEM((span, LANES), jnp.bfloat16),
        pltpu.VMEM((span, 2 * LANES), jnp.bfloat16),
    ]
    states = (f32(rows, LANES),) * 3

    def attend(blocks, steps, state, closing):
        info = jnp.stack([live] + [((mine - by) % spans) * span for by in steps]).astype(jnp.int32)
        operands = [info, query, *blocks, *(state or ())]
        out = (bf16(GROUP, frames + frames // 2, LANES),) if closing else states
        body = lambda *refs: attend_kernel(*refs, chunks=len(blocks), opening=state is None, closing=closing)
        extra = [pltpu.VMEM((rows, LANES), jnp.float32)] * 3 if closing else []
        return pl.pallas_call(
            body,
            name="attend%d" % len(blocks) + ("z" if closing else ""),
            out_shape=out,
            in_specs=[spec(SMEM)] + [spec(VMEM)] * (len(operands) - 1),
            out_specs=tuple(spec(VMEM) for _ in out),
            scratch_shapes=extra + scratch,
            compiler_params=params(40),
            cost_estimate=pl.CostEstimate(flops=4 * 10**9 * len(blocks), bytes_accessed=5 * 10**6, transcendentals=0),
        )(*operands)

    state = attend([kv], [0], None, False)
    state = attend(others[:2], [1, spans - 1], state, False)
    (mixed,) = attend(others[2:], [2], state, True)
    mixed = swap(mixed)
    attended, encoded = pl.pallas_call(
        output_kernel,
        name="output",
        out_shape=(bf16(frames, width),) * 2,
        in_specs=[spec(VMEM)] * 4,
        out_specs=(spec(VMEM),) * 2,
        compiler_params=params(20),
        cost_estimate=pl.CostEstimate(flops=10**9, bytes_accessed=4 * 10**6, transcendentals=0),
    )(mixed, out_weight, row(out_bias), stem)
    return attended, encoded


def solution(mesh):
    in_specs = (P(("dp", "seq"), None), P("dp"), P(), P(), P(), P(), P(), P(), P(), P(), P(), P())
    out_specs = (P(("dp", "seq"), None), P(("dp", "seq"), None))
    return jax.shard_map(shards, mesh=mesh, in_specs=in_specs, out_specs=out_specs, check_vma=False)
```

```python
import math

import jax
import jax.numpy as jnp
from jax import lax
from jax.experimental import pallas as pl
from jax.experimental.pallas import tpu as pltpu
from jax.sharding import PartitionSpec as P

HEAD_DIM = 64
LANES = 128
GROUP = 8
norm_epsilon = 1e-05


def turns(first_frame, frame_count, model_width):
    half_width = model_width // 2
    increment = math.log(10000.0) / (half_width - 1)
    inverse = jnp.exp(-increment * jnp.arange(half_width, dtype=jnp.float32))
    step = jnp.arange(16 + frame_count // 16, dtype=jnp.int32)
    moments = jnp.where(step < 16, step, first_frame + 16 * (step - 16)).astype(jnp.float32)
    angles = moments[:, None] * inverse[None, :]
    return jnp.sin(angles), jnp.cos(angles)


def gelu(v):
    return 0.5 * v * (1.0 + lax.erf(v * (2.0**-0.5)))


def window(whole, rolled, start):
    if start % LANES == 0:
        return whole[:, start : start + LANES]
    return rolled[:, start - 64 : start + 64]


def ab_start(g):
    return 320 * (g // 2) + 192 * (g % 2)


def s_start(g):
    return 320 * (g // 2) + 128


def low_lanes(rows):
    return lax.broadcasted_iota(jnp.int32, (rows, LANES), 1) < 64


def stem_kernel(
    first_ref, early_ref, mel_ref, late_ref, sin_ref, cos_ref,
    rows_ref, qv_ref, w1_hbm, w2_hbm, wp_hbm,
    kv_ref, q_ref, stem_ref,
    w1, w2, wp, odd, mel, around, sems,
):
    frames, width = stem_ref.shape
    c1 = pltpu.make_async_copy(w1_hbm, w1, sems.at[0])
    c1.start()
    part = w2.shape[0] // W2_PARTS
    c2 = []
    for i in range(W2_PARTS):
        rows = pl.ds(i * part, part)
        c2.append(pltpu.make_async_copy(w2_hbm.at[rows], w2.at[rows], sems.at[1 + i]))
        c2[-1].start()
    c3 = []
    for i, at in enumerate((1, 2, 0)):
        cols = pl.ds(width * at, width)
        c3.append(pltpu.make_async_copy(wp_hbm.at[:, cols], wp.at[:, cols], sems.at[1 + W2_PARTS + i]))
        c3[-1].start()
    b1, b2, gain, nbias = (rows_ref[pl.ds(i * width, width)].reshape(1, width) for i in range(4))
    pad = 16
    mel[...] = mel_ref[...].astype(jnp.float32)
    around[0:1, :LANES] = early_ref[0:1, :].astype(jnp.float32)
    around[0:1, LANES:] = early_ref[1:2, :].astype(jnp.float32)
    around[1 : frames + 1, :LANES] = mel[pl.ds(0, frames, stride=2), :]
    around[1 : frames + 1, LANES:] = mel[pl.ds(1, frames, stride=2), :]
    around[frames + 1 : frames + 2, :LANES] = late_ref[0:1, :].astype(jnp.float32)
    around[frames + 1 : frames + 2, LANES:] = late_ref[1:2, :].astype(jnp.float32)
    low_rows, mid_rows, high_rows = (around[i : i + frames, :].astype(jnp.bfloat16) for i in range(3))
    top = jnp.concatenate([around[0:pad, :], around[1 : pad + 1, :LANES]], axis=1).astype(jnp.bfloat16)
    lhs = jnp.concatenate(
        [
            top,
            jnp.concatenate([mid_rows, high_rows[:, :LANES]], axis=1),
            jnp.concatenate([low_rows[:, LANES:], mid_rows], axis=1),
        ],
        axis=0,
    )
    c1.wait()
    first = gelu(jnp.dot(lhs, w1[...], preferred_element_type=jnp.float32) + b1)
    odd[0:1, :] = jnp.where(first_ref[0] != 0, 0.0, first[0:1])
    odd[1 : frames + 1, :] = first[pad : pad + frames]
    before = odd[0:frames, :].astype(jnp.bfloat16)
    after = first[pad : pad + frames].astype(jnp.bfloat16)
    even = first[pad + frames :].astype(jnp.bfloat16)
    total = None
    per = W2_PARTS // 3
    for tap, rows in enumerate((before, even, after)):
        for i in range(per):
            c2[tap * per + i].wait()
            term = jnp.dot(
                rows[:, i * part : (i + 1) * part],
                w2[(tap * per + i) * part : (tap * per + i + 1) * part, :],
                preferred_element_type=jnp.float32,
            )
            total = term if total is None else total + term
    second = gelu(total + b2)
    fine_sin, fine_cos = sin_ref[0:16, :], cos_ref[0:16, :]
    for a in range(frames // 16):
        at = slice(16 * a, 16 * a + 16)
        s, c = sin_ref[16 + a : 17 + a, :], cos_ref[16 + a : 17 + a, :]
        half = width // 2
        stem_ref[at, :half] = (second[at, :half] + (s * fine_cos + c * fine_sin)).astype(jnp.bfloat16)
        stem_ref[at, half:] = (second[at, half:] + (c * fine_cos - s * fine_sin)).astype(jnp.bfloat16)
    wide = stem_ref[...].astype(jnp.float32)
    centred = wide - jnp.mean(wide, axis=1, keepdims=True)
    spread = jnp.mean(centred * centred, axis=1, keepdims=True)
    normed = (centred * lax.rsqrt(spread + norm_epsilon) * gain + nbias).astype(jnp.bfloat16)
    c3[0].wait()
    keys = jnp.dot(normed, wp[:, width : 2 * width], preferred_element_type=jnp.float32)
    c3[1].wait()
    values = jnp.dot(normed, wp[:, 2 * width :], preferred_element_type=jnp.float32) + qv_ref[1:2, :]
    keys_r = pltpu.roll(keys, width - 64, 1)
    values_r = pltpu.roll(values, width - 64, 1)
    low = low_lanes(frames)
    for g in range(GROUP):
        kv_ref[g, 0:frames, :] = window(keys, keys_r, ab_start(g)).astype(jnp.bfloat16)
        kv_ref[g, frames : 2 * frames, :] = window(values, values_r, ab_start(g)).astype(jnp.bfloat16)
        shared = jnp.where(low, window(keys, keys_r, s_start(g)), window(values, values_r, s_start(g) - 64))
        kv_ref[g, 2 * frames : 3 * frames, :] = shared.astype(jnp.bfloat16)


    c3[2].wait()
    half = frames // 2
    scale = HEAD_DIM**-0.5 * math.log2(math.e)
    q = jnp.dot(normed, wp[:, :width], preferred_element_type=jnp.float32)
    q = (q + qv_ref[0:1, :]) * scale
    q_r = pltpu.roll(q, width - 64, 1)
    low = low_lanes(half)
    for g in range(GROUP):
        q_ref[g, 0:frames, :] = window(q, q_r, ab_start(g)).astype(jnp.bfloat16)
        rows = slice(half * (g % 2), half * (g % 2 + 1))
        shared = window(q, q_r, s_start(g))[rows]
        q_ref[g, frames : frames + half, :] = jnp.where(low, shared, 0.0).astype(jnp.bfloat16)


NEG = -1e30
TILE = 256


def attend_kernel(*refs, parts, opening, closing):
    refs = list(refs)
    info = refs.pop(0)
    q_ref = refs.pop(0)
    chunks = [[refs.pop(0) for _ in range(n)] for n in parts]
    old = None if opening else [refs.pop(0) for _ in range(2)]
    o_ref = refs.pop(0) if closing else None
    m_ref, a_ref = refs.pop(0), refs.pop(0)
    qs, ks, vs, s0, s1, x0, x1 = refs
    units, rows, _ = qs.shape
    span = ks.shape[1]
    frames = span // GROUP
    half = frames // 2
    whole = GROUP

    if not opening:
        for new, was in zip((m_ref, a_ref), old):
            new[...] = was[...]

    low = low_lanes(frames)
    for j in range(GROUP):
        q = q_ref[j, 0:frames, :]
        qs[j, 0:frames, :] = jnp.where(low, q, jnp.zeros_like(q))
        qs[j, frames:rows, :] = jnp.where(low, jnp.zeros_like(q), q)
    for u in range(whole, units):
        few = rows // half
        qs[u] = q_ref[(u - whole) * few : (u - whole + 1) * few, frames : frames + half, :].reshape(rows, LANES)
    ones = jnp.ones((span, LANES), jnp.bfloat16)

    def scores(u, t):
        team = jnp.where(u < whole, 0, 1)
        return lax.dot_general(
            qs[u], ks[team, t * TILE : (t + 1) * TILE, :], (((1,), (1,)), ((), ())), preferred_element_type=jnp.float32
        )

    def lane_max(s):
        return jnp.maximum(s[:, :LANES], s[:, LANES:])

    def spread_max(top):
        return jnp.broadcast_to(jnp.max(top, axis=1, keepdims=True), top.shape)

    def begin(u, s_out, x_out):
        top = None
        for t in range(span // TILE):
            s = scores(u, t)
            s_out[:, t * TILE : (t + 1) * TILE] = s
            top = lane_max(s) if top is None else jnp.maximum(top, lane_max(s))
        x_out[...] = spread_max(top)

    def both(u, s_in, x_in, nxt, s_out, x_out, fresh):
        team = jnp.where(u < whole, 0, 1)
        if fresh:
            m_new = x_in[...]
        else:
            m_old = m_ref[u]
            m_new = jnp.maximum(m_old, x_in[...])
        m_two = jnp.concatenate([m_new, m_new], axis=1)
        m_ref[u] = m_new
        total, top = None, None
        for t in range(span // TILE):
            at = slice(t * TILE, (t + 1) * TILE)
            p = jnp.exp2(s_in[:, at] - m_two).astype(jnp.bfloat16)
            s = scores(nxt, t)
            s_out[:, at] = s
            top = lane_max(s) if top is None else jnp.maximum(top, lane_max(s))
            term = jnp.dot(p, vs[team, at, :], preferred_element_type=jnp.float32)
            total = term if total is None else total + term
        x_out[...] = spread_max(top)
        if fresh:
            a_ref[u] = total
        else:
            keep = jnp.exp2(m_old - m_new)
            a_ref[u] = a_ref[u] * jnp.concatenate([keep, keep], axis=1) + total

    for c, blocks in enumerate(chunks):
        live = info[0] - info[1 + c]
        fresh = opening and c == 0

        def gather(first, last):
            got = [kv[:, first:last, :] for kv in blocks]
            got = got[0] if len(got) == 1 else jnp.concatenate(got, axis=0)
            return got.reshape(span, LANES)

        @pl.when(live > 0)
        def _():
            ks[0] = gather(0, frames)
            shared = gather(2 * frames, 3 * frames)
            ks[1] = shared
            vs[0, :, :LANES] = gather(frames, 2 * frames)
            vs[1, :, :LANES] = shared
            vs[0, :, LANES:] = ones
            vs[1, :, LANES:] = ones

            @pl.when(live < span)
            def _():
                alive = lax.broadcasted_iota(jnp.int32, (span, LANES), 0) < live
                for team in range(2):
                    k = ks[team].astype(jnp.float32)
                    ks[team] = jnp.where(alive, k, k[0:1]).astype(jnp.bfloat16)
                    for side in range(2):
                        at = slice(side * LANES, (side + 1) * LANES)
                        v = vs[team, :, at].astype(jnp.float32)
                        vs[team, :, at] = jnp.where(alive, v, 0.0).astype(jnp.bfloat16)

            begin(0, s0, x0)

            def step(i, carry):
                both(2 * i, s0, x0, 2 * i + 1, s1, x1, fresh)
                both(2 * i + 1, s1, x1, jnp.minimum(2 * i + 2, units - 1), s0, x0, fresh)
                return carry

            lax.fori_loop(0, units // 2, step, 0)

        if fresh:

            @pl.when(live <= 0)
            def _():
                m_ref[...] = jnp.full(m_ref.shape, NEG, jnp.float32)
                a_ref[...] = jnp.zeros(a_ref.shape, jnp.float32)

    if closing:
        for u in range(units):
            o = a_ref[u, :, :LANES] / a_ref[u, :, LANES:]
            if u < whole:
                o_ref[u, 0:frames, :] = jnp.where(low, o[:frames], o[frames:]).astype(jnp.bfloat16)
            else:
                few = rows // half
                o = jnp.where(low_lanes(rows), 0.0, o).astype(jnp.bfloat16).reshape(few, half, LANES)
                o_ref[(u - whole) * few : (u - whole + 1) * few, frames : frames + half, :] = o


def output_kernel(o_ref, w_ref, bias_ref, stem_ref, attended_ref, encoded_ref):
    frames, width = stem_ref.shape
    half = frames // 2
    total = None
    for g in range(GROUP):
        at = ab_start(g)
        term = jnp.dot(o_ref[g, 0:frames, :], w_ref[at : at + LANES, :], preferred_element_type=jnp.float32)
        total = term if total is None else total + term
        if g % 2:
            at = s_start(g) - 64
            shared = jnp.concatenate(
                [o_ref[g - 1, frames : frames + half, :], o_ref[g, frames : frames + half, :]], axis=0
            )
            total = total + jnp.dot(shared, w_ref[at : at + LANES, :], preferred_element_type=jnp.float32)
    total = total + bias_ref[...]
    attended_ref[...] = total.astype(jnp.bfloat16)
    encoded_ref[...] = (stem_ref[...].astype(jnp.float32) + total).astype(jnp.bfloat16)


STEM_MIB = 60
W2_PARTS = 6
VMEM = pltpu.MemorySpace.VMEM
SMEM = pltpu.MemorySpace.SMEM


def spec(space):
    return pl.BlockSpec(memory_space=space)


def params(mib):
    return pltpu.CompilerParams(vmem_limit_bytes=mib * 2**20)


def shards(
    spectrum, valid_frames, inlet_weight, inlet_bias, stride_weight, stride_bias, norm_gain, norm_bias,
    projection_weight, query_value_bias, out_weight, out_bias,
):
    mel_rows, channels = spectrum.shape
    frames = mel_rows // 2
    width = projection_weight.shape[0]
    count = lax.axis_size("seq")
    me = lax.axis_index("seq")
    down = [(i, i + 1) for i in range(count - 1)]
    up = [(i + 1, i) for i in range(count - 1)]
    early = lax.ppermute(spectrum[mel_rows - 2 :], "seq", down)
    late = lax.ppermute(spectrum[:2], "seq", up)
    sines, cosines = turns(me * frames, frames, width)
    first = (me == 0).astype(jnp.int32).reshape(1)
    row = lambda v: v.reshape(1, width)
    bf16 = lambda *dims: jax.ShapeDtypeStruct(dims, jnp.bfloat16)
    f32 = lambda *dims: jax.ShapeDtypeStruct(dims, jnp.float32)

    kv, query, stem = pl.pallas_call(
        stem_kernel,
        name="stem",
        out_shape=(bf16(GROUP, 3 * frames, LANES), bf16(GROUP, frames + frames // 2, LANES), bf16(frames, width)),
        in_specs=[spec(SMEM)] + [spec(VMEM)] * 7 + [spec(pltpu.MemorySpace.HBM)] * 3,
        out_specs=(spec(VMEM),) * 3,
        scratch_shapes=[
            pltpu.VMEM((3 * channels, width), jnp.bfloat16),
            pltpu.VMEM((3 * width, width), jnp.bfloat16),
            pltpu.VMEM((width, 3 * width), jnp.bfloat16),
            pltpu.VMEM((frames + 8, width), jnp.float32),
            pltpu.VMEM((mel_rows, channels), jnp.float32),
            pltpu.VMEM((frames + 8, 2 * channels), jnp.float32),
            pltpu.SemaphoreType.DMA((4 + W2_PARTS,)),
        ],
        compiler_params=params(STEM_MIB),
        cost_estimate=pl.CostEstimate(flops=4 * 10**9, bytes_accessed=20 * 10**6, transcendentals=0),
    )(
        first, early, spectrum, late, sines, cosines,
        jnp.concatenate([inlet_bias, stride_bias, norm_gain, norm_bias]), query_value_bias,
        inlet_weight.reshape(3 * channels, width), stride_weight.reshape(3 * width, width), projection_weight,
    )

    teams = [list(range(i, i + GROUP)) for i in range(0, count, GROUP)]
    swap = lambda v: lax.all_to_all(v, "seq", 0, 0, axis_index_groups=teams)
    kv = swap(kv)
    spans = count // GROUP
    shift = lambda v, by: lax.ppermute(v, "seq", [(i, (i + by * GROUP) % count) for i in range(count)])
    below, above = shift(kv, 1), shift(kv, spans - 1)
    cut = GROUP // 2
    far = [shift(below[:cut], 1), shift(above[cut:], spans - 1)]

    query = swap(query)

    live = valid_frames[0]
    mine = me // GROUP
    span = GROUP * frames
    rows = 2 * frames
    units = GROUP + GROUP // 4
    scratch = [
        pltpu.VMEM((units, rows, LANES), jnp.bfloat16),
        pltpu.VMEM((2, span, LANES), jnp.bfloat16),
        pltpu.VMEM((2, span, 2 * LANES), jnp.bfloat16),
        pltpu.VMEM((rows, span), jnp.float32),
        pltpu.VMEM((rows, span), jnp.float32),
        pltpu.VMEM((rows, LANES), jnp.float32),
        pltpu.VMEM((rows, LANES), jnp.float32),
    ]
    shapes = ((units, rows, LANES), (units, rows, 2 * LANES))

    def attend(chunks, steps, state, closing):
        info = jnp.stack([live] + [((mine - by) % spans) * span for by in steps]).astype(jnp.int32)
        operands = [info, query, *(b for c in chunks for b in c), *(state or ())]
        out = (bf16(GROUP, frames + frames // 2, LANES),) if closing else tuple(f32(*s) for s in shapes)
        parts = tuple(len(c) for c in chunks)
        body = lambda *refs: attend_kernel(*refs, parts=parts, opening=state is None, closing=closing)
        extra = [pltpu.VMEM(s, jnp.float32) for s in shapes] if closing else []
        return pl.pallas_call(
            body,
            name="attend%d" % len(chunks) + ("z" if closing else ""),
            out_shape=out,
            in_specs=[spec(SMEM)] + [spec(VMEM)] * (len(operands) - 1),
            out_specs=tuple(spec(VMEM) for _ in out),
            scratch_shapes=extra + scratch,
            compiler_params=params(48),
            cost_estimate=pl.CostEstimate(flops=4 * 10**9 * len(chunks), bytes_accessed=5 * 10**6, transcendentals=0),
        )(*operands)

    state = attend([[kv]], [0], None, False)
    state = attend([[below], [above]], [1, spans - 1], state, False)
    (mixed,) = attend([far], [2], state, True)
    mixed = swap(mixed)
    attended, encoded = pl.pallas_call(
        output_kernel,
        name="output",
        out_shape=(bf16(frames, width),) * 2,
        in_specs=[spec(VMEM)] * 4,
        out_specs=(spec(VMEM),) * 2,
        compiler_params=params(20),
        cost_estimate=pl.CostEstimate(flops=10**9, bytes_accessed=4 * 10**6, transcendentals=0),
    )(mixed, out_weight, row(out_bias), stem)
    return attended, encoded


def solution(mesh):
    in_specs = (P(("dp", "seq"), None), P("dp"), P(), P(), P(), P(), P(), P(), P(), P(), P(), P())
    out_specs = (P(("dp", "seq"), None), P(("dp", "seq"), None))
    return jax.shard_map(shards, mesh=mesh, in_specs=in_specs, out_specs=out_specs, check_vma=False)
```

```python
import math

import jax
import jax.numpy as jnp
from jax import lax
from jax.experimental import pallas as pl
from jax.experimental.pallas import tpu as pltpu
from jax.sharding import PartitionSpec as P

HEAD_DIM = 64
LANES = 128
GROUP = 8
norm_epsilon = 1e-05


def turns(first_frame, frame_count, model_width):
    half_width = model_width // 2
    increment = math.log(10000.0) / (half_width - 1)
    inverse = jnp.exp(-increment * jnp.arange(half_width, dtype=jnp.float32))
    step = jnp.arange(16 + frame_count // 16, dtype=jnp.int32)
    moments = jnp.where(step < 16, step, first_frame + 16 * (step - 16)).astype(jnp.float32)
    angles = moments[:, None] * inverse[None, :]
    return jnp.sin(angles), jnp.cos(angles)


def gelu(v):
    return 0.5 * v * (1.0 + lax.erf(v * (2.0**-0.5)))


def window(whole, rolled, start):
    if start % LANES == 0:
        return whole[:, start : start + LANES]
    return rolled[:, start - 64 : start + 64]


def ab_start(g):
    return 320 * (g // 2) + 192 * (g % 2)


def s_start(g):
    return 320 * (g // 2) + 128


def low_lanes(rows):
    return lax.broadcasted_iota(jnp.int32, (rows, LANES), 1) < 64


HOPS = ((0, 0), (0, 1), (0, 3), (1, 0), (1, 1), (1, 3), (0, 2), (1, 2))


def member(me, r, sign):
    dz, dx = HOPS[r]
    j = lax.rem(me, GROUP)
    return lax.rem(j // 4 + dz, 2) * 4 + lax.rem(lax.rem(j, 4) + 4 + sign * dx, 4)


def stem_kernel(
    info_ref, early_ref, mel_ref, late_ref, sin_ref, cos_ref,
    rows_ref, qv_ref, w1_hbm, w2_hbm, wp_hbm,
    *refs,
):
    out_refs, (normed_ref, stem_ref) = refs[:GROUP], refs[GROUP : GROUP + 2]
    w1, w2, wp, odd, mel, around, msg, sems = refs[GROUP + 2 :]
    frames, width = stem_ref.shape
    c1 = pltpu.make_async_copy(w1_hbm, w1, sems.at[0])
    c1.start()
    part = w2.shape[0] // W2_PARTS
    c2 = []
    for i in range(W2_PARTS):
        rows = pl.ds(i * part, part)
        c2.append(pltpu.make_async_copy(w2_hbm.at[rows], w2.at[rows], sems.at[1 + i]))
        c2[-1].start()
    c3 = []
    for i in range(2):
        there, here = pl.ds(width * (i + 1), width), pl.ds(width * i, width)
        c3.append(pltpu.make_async_copy(wp_hbm.at[:, there], wp.at[:, here], sems.at[1 + W2_PARTS + i]))
        c3[-1].start()
    b1, b2, gain, nbias = (rows_ref[pl.ds(i * width, width)].reshape(1, width) for i in range(4))
    pad = 16
    mel[...] = mel_ref[...].astype(jnp.float32)
    around[0:1, :LANES] = early_ref[0:1, :].astype(jnp.float32)
    around[0:1, LANES:] = early_ref[1:2, :].astype(jnp.float32)
    around[1 : frames + 1, :LANES] = mel[pl.ds(0, frames, stride=2), :]
    around[1 : frames + 1, LANES:] = mel[pl.ds(1, frames, stride=2), :]
    around[frames + 1 : frames + 2, :LANES] = late_ref[0:1, :].astype(jnp.float32)
    around[frames + 1 : frames + 2, LANES:] = late_ref[1:2, :].astype(jnp.float32)
    low_rows, mid_rows, high_rows = (around[i : i + frames, :].astype(jnp.bfloat16) for i in range(3))
    top = jnp.concatenate([around[0:pad, :], around[1 : pad + 1, :LANES]], axis=1).astype(jnp.bfloat16)
    lhs = jnp.concatenate(
        [
            top,
            jnp.concatenate([mid_rows, high_rows[:, :LANES]], axis=1),
            jnp.concatenate([low_rows[:, LANES:], mid_rows], axis=1),
        ],
        axis=0,
    )
    c1.wait()
    first = gelu(jnp.dot(lhs, w1[...], preferred_element_type=jnp.float32) + b1)
    odd[0:1, :] = jnp.where(info_ref[1] == 0, 0.0, first[0:1])
    odd[1 : frames + 1, :] = first[pad : pad + frames]
    before = odd[0:frames, :].astype(jnp.bfloat16)
    after = first[pad : pad + frames].astype(jnp.bfloat16)
    even = first[pad + frames :].astype(jnp.bfloat16)
    total = None
    per = W2_PARTS // 3
    for tap, rows in enumerate((before, even, after)):
        for i in range(per):
            c2[tap * per + i].wait()
            term = jnp.dot(
                rows[:, i * part : (i + 1) * part],
                w2[(tap * per + i) * part : (tap * per + i + 1) * part, :],
                preferred_element_type=jnp.float32,
            )
            total = term if total is None else total + term
    second = gelu(total + b2)
    fine_sin, fine_cos = sin_ref[0:16, :], cos_ref[0:16, :]
    for a in range(frames // 16):
        at = slice(16 * a, 16 * a + 16)
        s, c = sin_ref[16 + a : 17 + a, :], cos_ref[16 + a : 17 + a, :]
        half = width // 2
        stem_ref[at, :half] = (second[at, :half] + (s * fine_cos + c * fine_sin)).astype(jnp.bfloat16)
        stem_ref[at, half:] = (second[at, half:] + (c * fine_cos - s * fine_sin)).astype(jnp.bfloat16)
    wide = stem_ref[...].astype(jnp.float32)
    centred = wide - jnp.mean(wide, axis=1, keepdims=True)
    spread = jnp.mean(centred * centred, axis=1, keepdims=True)
    normed = (centred * lax.rsqrt(spread + norm_epsilon) * gain + nbias).astype(jnp.bfloat16)
    c3[0].wait()
    keys = jnp.dot(normed, wp[:, :width], preferred_element_type=jnp.float32)
    c3[1].wait()
    values = jnp.dot(normed, wp[:, width:], preferred_element_type=jnp.float32) + qv_ref[1:2, :]
    keys_r = pltpu.roll(keys, width - 64, 1)
    values_r = pltpu.roll(values, width - 64, 1)
    low = low_lanes(frames)
    at_k = 0
    for g in range(GROUP):
        msg[g, at_k : at_k + frames, :] = window(keys, keys_r, ab_start(g)).astype(jnp.bfloat16)
        msg[g, at_k + frames : at_k + 2 * frames, :] = window(values, values_r, ab_start(g)).astype(jnp.bfloat16)
        shared = jnp.where(low, window(keys, keys_r, s_start(g)), window(values, values_r, s_start(g) - 64))
        msg[g, at_k + 2 * frames : at_k + 3 * frames, :] = shared.astype(jnp.bfloat16)


    normed_ref[...] = normed
    for r, out in enumerate(out_refs):
        out[...] = msg[member(info_ref[1], r, 1)]


def query_kernel(normed_ref, qv_ref, wp_hbm, q_ref, w, sem):
    frames, width = normed_ref.shape
    half = frames // 2
    copy = pltpu.make_async_copy(wp_hbm.at[:, pl.ds(0, width)], w, sem)
    copy.start()
    copy.wait()
    scale = HEAD_DIM**-0.5 * math.log2(math.e)
    q = (jnp.dot(normed_ref[...], w[...], preferred_element_type=jnp.float32) + qv_ref[0:1, :]) * scale
    q_r = pltpu.roll(q, width - 64, 1)
    low = low_lanes(half)
    for g in range(GROUP):
        q_ref[g, 0:frames, :] = window(q, q_r, ab_start(g)).astype(jnp.bfloat16)
        rows = slice(half * (g % 2), half * (g % 2 + 1))
        shared = window(q, q_r, s_start(g))[rows]
        q_ref[g, frames : frames + half, :] = jnp.where(low, shared, 0.0).astype(jnp.bfloat16)


def pack_kernel(*refs):
    out = refs[-1]
    for i in range(out.shape[0]):
        out[i] = refs[i][refs[i].shape[0] - out.shape[1] :, :]


NEG = -1e30
TILE = 256


def attend_kernel(*refs, chunks, sources, opening, closing):
    refs = list(refs)
    info = refs.pop(0)
    q_ref = refs.pop(0)
    kv_refs = [refs.pop(0) for _ in range(sources)]
    old = None if opening else [refs.pop(0) for _ in range(2)]
    o_ref = refs.pop(0) if closing else None
    m_ref, a_ref = refs.pop(0), refs.pop(0)
    qs, ks, vs, s0, s1, x0, x1 = refs
    units, rows, _ = qs.shape
    span = ks.shape[1]
    frames = span // GROUP
    half = frames // 2
    whole = GROUP
    at_k = frames + half
    limit, me = info[0], info[1]
    spans = 4

    low = low_lanes(frames)
    for j in range(GROUP):
        q = q_ref[j, 0:frames, :]
        qs[j, 0:frames, :] = jnp.where(low, q, jnp.zeros_like(q))
        qs[j, frames:rows, :] = jnp.where(low, jnp.zeros_like(q), q)
    for u in range(whole, units):
        for k in range(rows // half):
            qs[u, k * half : (k + 1) * half, :] = q_ref[(u - whole) * (rows // half) + k, frames:at_k, :]
    ones = jnp.ones((span, LANES), jnp.bfloat16)

    def scores(u, t):
        team = jnp.where(u < whole, 0, 1)
        return lax.dot_general(
            qs[u], ks[team, t * TILE : (t + 1) * TILE, :], (((1,), (1,)), ((), ())), preferred_element_type=jnp.float32
        )

    def lane_max(s):
        return jnp.maximum(s[:, :LANES], s[:, LANES:])

    def spread_max(top):
        return jnp.broadcast_to(jnp.max(top, axis=1, keepdims=True), top.shape)

    def begin(u, s_out, x_out):
        top = None
        for t in range(span // TILE):
            s = scores(u, t)
            s_out[:, t * TILE : (t + 1) * TILE] = s
            top = lane_max(s) if top is None else jnp.maximum(top, lane_max(s))
        x_out[...] = spread_max(top)

    def both(u, s_in, x_in, nxt, s_out, x_out, fresh, was):
        team = jnp.where(u < whole, 0, 1)
        if fresh:
            m_new = x_in[...]
        else:
            m_old = was[0][u]
            m_new = jnp.maximum(m_old, x_in[...])
        m_two = jnp.concatenate([m_new, m_new], axis=1)
        m_ref[u] = m_new
        total, top = None, None
        for t in range(span // TILE):
            at = slice(t * TILE, (t + 1) * TILE)
            p = jnp.exp2(s_in[:, at] - m_two).astype(jnp.bfloat16)
            s = scores(nxt, t)
            s_out[:, at] = s
            top = lane_max(s) if top is None else jnp.maximum(top, lane_max(s))
            term = jnp.dot(p, vs[team, at, :], preferred_element_type=jnp.float32)
            total = term if total is None else total + term
        x_out[...] = spread_max(top)
        if fresh:
            a_ref[u] = total
        else:
            keep = jnp.exp2(m_old - m_new)
            a_ref[u] = was[1][u] * jnp.concatenate([keep, keep], axis=1) + total

    for c, blocks in enumerate(chunks):
        fresh = opening and c == 0
        was = old if c == 0 else (m_ref, a_ref)
        starts = [
            lax.rem(me // GROUP + spans - up, spans) * span + member(me, hop, -1) * frames for _, _, hop, up in blocks
        ]
        lowest, at_low, highest = starts[0], 0, starts[0]
        for i, start in enumerate(starts[1:], 1):
            at_low = jnp.where(start < lowest, i * frames, at_low)
            lowest = jnp.minimum(lowest, start)
            highest = jnp.maximum(highest, start)

        @pl.when(limit > lowest)
        def _():
            for i, (source, index, _, _) in enumerate(blocks):
                at = slice(i * frames, (i + 1) * frames)
                kv = kv_refs[source]
                part = lambda n: kv[index, n * frames : (n + 1) * frames, :]
                ks[0, at, :] = part(0)
                ks[1, at, :] = part(2)
                vs[0, at, :LANES] = part(1)
                vs[1, at, :LANES] = part(2)
            vs[0, :, LANES:] = ones
            vs[1, :, LANES:] = ones

            @pl.when(limit < highest + frames)
            def _():
                row = lax.broadcasted_iota(jnp.int32, (frames, LANES), 0)
                for team in range(2):
                    spare = ks[team, pl.ds(pl.multiple_of(at_low, frames), 16), :].astype(jnp.float32)[0:1]
                    for i, start in enumerate(starts):
                        at = slice(i * frames, (i + 1) * frames)
                        alive = row < limit - start
                        k = ks[team, at, :].astype(jnp.float32)
                        ks[team, at, :] = jnp.where(alive, k, spare).astype(jnp.bfloat16)
                        for side in range(2):
                            lanes = slice(side * LANES, (side + 1) * LANES)
                            v = vs[team, at, lanes].astype(jnp.float32)
                            vs[team, at, lanes] = jnp.where(alive, v, 0.0).astype(jnp.bfloat16)

            begin(0, s0, x0)

            def step(i, carry):
                both(2 * i, s0, x0, 2 * i + 1, s1, x1, fresh, was)
                both(2 * i + 1, s1, x1, jnp.minimum(2 * i + 2, units - 1), s0, x0, fresh, was)
                return carry

            lax.fori_loop(0, units // 2, step, 0)

        if c == 0:

            @pl.when(limit <= lowest)
            def _():
                if fresh:
                    m_ref[...] = jnp.full(m_ref.shape, NEG, jnp.float32)
                    a_ref[...] = jnp.zeros(a_ref.shape, jnp.float32)
                else:
                    m_ref[...] = was[0][...]
                    a_ref[...] = was[1][...]

    if closing:
        for u in range(units):
            o = a_ref[u, :, :LANES] / a_ref[u, :, LANES:]
            if u < whole:
                o_ref[u, 0:frames, :] = jnp.where(low, o[:frames], o[frames:]).astype(jnp.bfloat16)
            else:
                o = jnp.where(low_lanes(rows), 0.0, o).astype(jnp.bfloat16)
                for k in range(rows // half):
                    place = (u - whole) * (rows // half) + k
                    o_ref[place, frames:at_k, :] = o[k * half : (k + 1) * half]


def output_kernel(o_ref, w_ref, bias_ref, stem_ref, attended_ref, encoded_ref):
    frames, width = stem_ref.shape
    half = frames // 2
    total = None
    for g in range(GROUP):
        at = ab_start(g)
        term = jnp.dot(o_ref[g, 0:frames, :], w_ref[at : at + LANES, :], preferred_element_type=jnp.float32)
        total = term if total is None else total + term
        if g % 2:
            at = s_start(g) - 64
            shared = jnp.concatenate(
                [o_ref[g - 1, frames : frames + half, :], o_ref[g, frames : frames + half, :]], axis=0
            )
            total = total + jnp.dot(shared, w_ref[at : at + LANES, :], preferred_element_type=jnp.float32)
    total = total + bias_ref[...]
    attended_ref[...] = total.astype(jnp.bfloat16)
    encoded_ref[...] = (stem_ref[...].astype(jnp.float32) + total).astype(jnp.bfloat16)


STEM_MIB = 60
W2_PARTS = 6
VMEM = pltpu.MemorySpace.VMEM
SMEM = pltpu.MemorySpace.SMEM


def spec(space):
    return pl.BlockSpec(memory_space=space)


def params(mib):
    return pltpu.CompilerParams(vmem_limit_bytes=mib * 2**20)


def shards(
    spectrum, valid_frames, inlet_weight, inlet_bias, stride_weight, stride_bias, norm_gain, norm_bias,
    projection_weight, query_value_bias, out_weight, out_bias,
):
    mel_rows, channels = spectrum.shape
    frames = mel_rows // 2
    width = projection_weight.shape[0]
    count = lax.axis_size("seq")
    me = lax.axis_index("seq")
    down = [(i, i + 1) for i in range(count - 1)]
    up = [(i + 1, i) for i in range(count - 1)]
    early = lax.ppermute(spectrum[mel_rows - 2 :], "seq", down)
    late = lax.ppermute(spectrum[:2], "seq", up)
    sines, cosines = turns(me * frames, frames, width)
    info = jnp.stack([valid_frames[0], me]).astype(jnp.int32)
    row = lambda v: v.reshape(1, width)
    bf16 = lambda *dims: jax.ShapeDtypeStruct(dims, jnp.bfloat16)
    f32 = lambda *dims: jax.ShapeDtypeStruct(dims, jnp.float32)

    *messages, normed, stem = pl.pallas_call(
        stem_kernel,
        name="stem",
        out_shape=(bf16(3 * frames, LANES),) * GROUP + (bf16(frames, width),) * 2,
        in_specs=[spec(SMEM)] + [spec(VMEM)] * 7 + [spec(pltpu.MemorySpace.HBM)] * 3,
        out_specs=(spec(VMEM),) * (GROUP + 2),
        scratch_shapes=[
            pltpu.VMEM((3 * channels, width), jnp.bfloat16),
            pltpu.VMEM((3 * width, width), jnp.bfloat16),
            pltpu.VMEM((width, 2 * width), jnp.bfloat16),
            pltpu.VMEM((frames + 8, width), jnp.float32),
            pltpu.VMEM((mel_rows, channels), jnp.float32),
            pltpu.VMEM((frames + 8, 2 * channels), jnp.float32),
            pltpu.VMEM((GROUP, 3 * frames, LANES), jnp.bfloat16),
            pltpu.SemaphoreType.DMA((4 + W2_PARTS,)),
        ],
        compiler_params=params(STEM_MIB),
        cost_estimate=pl.CostEstimate(flops=4 * 10**9, bytes_accessed=20 * 10**6, transcendentals=0),
    )(
        info, early, spectrum, late, sines, cosines,
        jnp.concatenate([inlet_bias, stride_bias, norm_gain, norm_bias]), query_value_bias,
        inlet_weight.reshape(3 * channels, width), stride_weight.reshape(3 * width, width), projection_weight,
    )

    spans = count // GROUP

    def send(v, r):
        dz, dx = HOPS[r]
        there = lambda i: i // 8 * 8 + (i // 4 + dz) % 2 * 4 + (i + dx) % 4
        return lax.ppermute(v, "seq", [(i, there(i)) for i in range(count)])

    def shift(v, by):
        return lax.ppermute(v, "seq", [(i, (i + by * GROUP) % count) for i in range(count)])

    def pack(parts, after):
        return pl.pallas_call(
            pack_kernel,
            name="pack",
            out_shape=bf16(len(parts), 3 * frames, LANES),
            in_specs=[spec(VMEM)] * len(parts) + [spec(pl.ANY)] * len(after),
            out_specs=spec(VMEM),
            compiler_params=params(4),
            cost_estimate=pl.CostEstimate(flops=10**8, bytes_accessed=10**6, transcendentals=0),
        )(*parts, *after)

    blocks = [messages[0]] + [send(messages[r], r) for r in range(1, GROUP)]
    cut = GROUP // 2
    query = pl.pallas_call(
        query_kernel,
        name="query",
        out_shape=bf16(GROUP, frames + frames // 2, LANES),
        in_specs=[spec(VMEM), spec(VMEM), spec(pltpu.MemorySpace.HBM)],
        out_specs=spec(VMEM),
        scratch_shapes=[pltpu.VMEM((width, width), jnp.bfloat16), pltpu.SemaphoreType.DMA],
        compiler_params=params(60),
        cost_estimate=pl.CostEstimate(flops=10**9, bytes_accessed=4 * 10**6, transcendentals=0),
    )(normed, query_value_bias, projection_weight)
    own = pack(blocks, [query])
    below, above = shift(own, 1), shift(own, spans - 1)
    far = shift(below[:cut], 1), shift(above[cut:], spans - 1)
    teams = [list(range(i, i + GROUP)) for i in range(0, count, GROUP)]
    swap = lambda v: lax.all_to_all(v, "seq", 0, 0, axis_index_groups=teams)
    query = swap(query)

    span = GROUP * frames
    rows = 2 * frames
    units = GROUP + GROUP // 4
    scratch = [
        pltpu.VMEM((units, rows, LANES), jnp.bfloat16),
        pltpu.VMEM((2, span, LANES), jnp.bfloat16),
        pltpu.VMEM((2, span, 2 * LANES), jnp.bfloat16),
        pltpu.VMEM((rows, span), jnp.float32),
        pltpu.VMEM((rows, span), jnp.float32),
        pltpu.VMEM((rows, LANES), jnp.float32),
        pltpu.VMEM((rows, LANES), jnp.float32),
    ]
    shapes = ((units, rows, LANES), (units, rows, 2 * LANES))

    def attend(chunks, arrays, state, closing):
        operands = [info, query, *arrays, *(state or ())]
        out = (bf16(GROUP, frames + frames // 2, LANES),) if closing else tuple(f32(*s) for s in shapes)
        body = lambda *refs: attend_kernel(
            *refs, chunks=chunks, sources=len(arrays), opening=state is None, closing=closing
        )
        extra = [pltpu.VMEM(s, jnp.float32) for s in shapes] if closing else []
        return pl.pallas_call(
            body,
            name="attend%d" % len(chunks) + ("z" if closing else ""),
            out_shape=out,
            in_specs=[spec(SMEM)] + [spec(VMEM)] * (len(operands) - 1),
            out_specs=tuple(spec(VMEM) for _ in out),
            scratch_shapes=extra + scratch,
            compiler_params=params(30),
            cost_estimate=pl.CostEstimate(flops=4 * 10**9 * len(chunks), bytes_accessed=5 * 10**6, transcendentals=0),
        )(*operands)

    lows, highs = range(cut), range(cut, GROUP)
    chunk = lambda source, up: [(source, r, r, up) for r in range(GROUP)]
    last = [(0, r, r, 2) for r in lows] + [(1, r - cut, r, 2) for r in highs]
    state = attend([chunk(0, 0)], [own], None, False)
    state = attend([chunk(0, 1), chunk(1, spans - 1)], [below, above], state, False)
    (mixed,) = attend([last], far, state, True)
    mixed = swap(mixed)
    attended, encoded = pl.pallas_call(
        output_kernel,
        name="output",
        out_shape=(bf16(frames, width),) * 2,
        in_specs=[spec(VMEM)] * 4,
        out_specs=(spec(VMEM),) * 2,
        compiler_params=params(20),
        cost_estimate=pl.CostEstimate(flops=10**9, bytes_accessed=4 * 10**6, transcendentals=0),
    )(mixed, out_weight, row(out_bias), stem)
    return attended, encoded


def solution(mesh):
    in_specs = (P(("dp", "seq"), None), P("dp"), P(), P(), P(), P(), P(), P(), P(), P(), P(), P())
    out_specs = (P(("dp", "seq"), None), P(("dp", "seq"), None))
    return jax.shard_map(shards, mesh=mesh, in_specs=in_specs, out_specs=out_specs, check_vma=False)
```

```python
import math

import jax
import jax.numpy as jnp
from jax import lax
from jax.experimental import pallas as pl
from jax.experimental.pallas import tpu as pltpu
from jax.sharding import PartitionSpec as P


HEAD_DIM = 64
LANES = 128
GROUP = 8
norm_epsilon = 1e-05


def turns(first_frame, frame_count, model_width):
    half_width = model_width // 2
    increment = math.log(10000.0) / (half_width - 1)
    dims = (16 + frame_count // 16 + 6, half_width)
    column = lax.broadcasted_iota(jnp.int32, dims, 1).astype(jnp.float32)
    step = lax.broadcasted_iota(jnp.int32, dims, 0)
    moments = jnp.where(step < 16, step, first_frame + 16 * (step - 16)).astype(jnp.float32)
    angles = moments * jnp.exp(-increment * column)
    return jnp.sin(angles), jnp.cos(angles)


def gelu(v):
    return 0.5 * v * (1.0 + lax.erf(v * (2.0**-0.5)))


def window(whole, rolled, start):
    if start % LANES == 0:
        return whole[:, start : start + LANES]
    return rolled[:, start - 64 : start + 64]


def ab_start(g):
    return 320 * (g // 2) + 192 * (g % 2)


def s_start(g):
    return 320 * (g // 2) + 128


def low_lanes(rows):
    return lax.broadcasted_iota(jnp.int32, (rows, LANES), 1) < 64


HOPS = ((0, 0), (0, 1), (0, 3), (0, 2), (1, 0), (1, 1), (1, 3), (1, 2))


def member(me, r, sign):
    dz, dx = HOPS[r]
    j = lax.rem(me, GROUP)
    return lax.rem(j // 4 + dz, 2) * 4 + lax.rem(lax.rem(j, 4) + 4 + sign * dx, 4)


def stem_kernel(
    me_ref, early_ref, late_ref, mel_ref, b1_ref, b2_ref, gain_ref, nbias_ref, qv_ref, w1_hbm, w2_hbm, wp_hbm,
    *refs,
):
    out_refs, stem_ref = refs[:GROUP], refs[GROUP]
    w1, w2, wp, odd, mel, around, msg, sems = refs[GROUP + 1 :]
    frames, width = stem_ref.shape
    c1 = pltpu.make_async_copy(w1_hbm, w1, sems.at[0])
    c1.start()
    part = w2.shape[0] // W2_PARTS
    c2 = []
    for i in range(W2_PARTS):
        rows = pl.ds(i * part, part)
        c2.append(pltpu.make_async_copy(w2_hbm.at[rows], w2.at[rows], sems.at[1 + i]))
        c2[-1].start()
    c3 = []
    for i, at in enumerate((1, 2, 0)):
        cols = pl.ds(width * at, width)
        c3.append(pltpu.make_async_copy(wp_hbm.at[:, cols], wp.at[:, cols], sems.at[1 + W2_PARTS + i]))
        c3[-1].start()
    b1, b2, gain, nbias = (r[...].reshape(1, width) for r in (b1_ref, b2_ref, gain_ref, nbias_ref))
    pad = 16
    mel[...] = mel_ref[...].astype(jnp.float32)
    around[0:1, :LANES] = early_ref[0:1, :].astype(jnp.float32)
    around[0:1, LANES:] = early_ref[1:2, :].astype(jnp.float32)
    around[1 : frames + 1, :LANES] = mel[pl.ds(0, frames, stride=2), :]
    around[1 : frames + 1, LANES:] = mel[pl.ds(1, frames, stride=2), :]
    around[frames + 1 : frames + 2, :LANES] = late_ref[0:1, :].astype(jnp.float32)
    around[frames + 1 : frames + 2, LANES:] = late_ref[1:2, :].astype(jnp.float32)
    low_rows, mid_rows, high_rows = (around[i : i + frames, :].astype(jnp.bfloat16) for i in range(3))
    top = jnp.concatenate([around[0:pad, :], around[1 : pad + 1, :LANES]], axis=1).astype(jnp.bfloat16)
    lhs = jnp.concatenate(
        [
            top,
            jnp.concatenate([mid_rows, high_rows[:, :LANES]], axis=1),
            jnp.concatenate([low_rows[:, LANES:], mid_rows], axis=1),
        ],
        axis=0,
    )
    sines, cosines = turns(me_ref[0] * frames, frames, width)
    c1.wait()
    first = gelu(jnp.dot(lhs, w1[...], preferred_element_type=jnp.float32) + b1)
    odd[0:1, :] = jnp.where(me_ref[0] == 0, 0.0, first[0:1])
    odd[1 : frames + 1, :] = first[pad : pad + frames]
    before = odd[0:frames, :].astype(jnp.bfloat16)
    after = first[pad : pad + frames].astype(jnp.bfloat16)
    even = first[pad + frames :].astype(jnp.bfloat16)
    total = None
    per = W2_PARTS // 3
    for tap, rows in enumerate((before, even, after)):
        for i in range(per):
            c2[tap * per + i].wait()
            term = jnp.dot(
                rows[:, i * part : (i + 1) * part],
                w2[(tap * per + i) * part : (tap * per + i + 1) * part, :],
                preferred_element_type=jnp.float32,
            )
            total = term if total is None else total + term
    second = gelu(total + b2)
    fine_sin, fine_cos = sines[0:16, :], cosines[0:16, :]
    for a in range(frames // 16):
        at = slice(16 * a, 16 * a + 16)
        s, c = sines[16 + a : 17 + a, :], cosines[16 + a : 17 + a, :]
        half = width // 2
        stem_ref[at, :half] = (second[at, :half] + (s * fine_cos + c * fine_sin)).astype(jnp.bfloat16)
        stem_ref[at, half:] = (second[at, half:] + (c * fine_cos - s * fine_sin)).astype(jnp.bfloat16)
    wide = stem_ref[...].astype(jnp.float32)
    centred = wide - jnp.mean(wide, axis=1, keepdims=True)
    spread = jnp.mean(centred * centred, axis=1, keepdims=True)
    normed = (centred * lax.rsqrt(spread + norm_epsilon) * gain + nbias).astype(jnp.bfloat16)
    c3[0].wait()
    keys = jnp.dot(normed, wp[:, width : 2 * width], preferred_element_type=jnp.float32)
    c3[1].wait()
    values = jnp.dot(normed, wp[:, 2 * width :], preferred_element_type=jnp.float32) + qv_ref[1:2, :]
    keys_r = pltpu.roll(keys, width - 64, 1)
    values_r = pltpu.roll(values, width - 64, 1)
    low = low_lanes(frames)
    at_k = frames + frames // 2
    for g in range(GROUP):
        msg[g, at_k : at_k + frames, :] = window(keys, keys_r, ab_start(g)).astype(jnp.bfloat16)
        msg[g, at_k + frames : at_k + 2 * frames, :] = window(values, values_r, ab_start(g)).astype(jnp.bfloat16)
        shared = jnp.where(low, window(keys, keys_r, s_start(g)), window(values, values_r, s_start(g) - 64))
        msg[g, at_k + 2 * frames : at_k + 3 * frames, :] = shared.astype(jnp.bfloat16)


    c3[2].wait()
    half = frames // 2
    scale = HEAD_DIM**-0.5 * math.log2(math.e)
    q = jnp.dot(normed, wp[:, :width], preferred_element_type=jnp.float32)
    q = (q + qv_ref[0:1, :]) * scale
    q_r = pltpu.roll(q, width - 64, 1)
    low = low_lanes(half)
    for g in range(GROUP):
        msg[g, 0:frames, :] = window(q, q_r, ab_start(g)).astype(jnp.bfloat16)
        rows = slice(half * (g % 2), half * (g % 2 + 1))
        shared = window(q, q_r, s_start(g))[rows]
        msg[g, frames : frames + half, :] = jnp.where(low, shared, 0.0).astype(jnp.bfloat16)
    for r, out in enumerate(out_refs):
        out[...] = msg[member(me_ref[0], r, 1)]


def pack_kernel(*refs):
    kv, q = refs[-2:]
    for i in range(kv.shape[0]):
        q[i] = refs[i][: q.shape[1], :]
        kv[i] = refs[i][q.shape[1] :, :]


NEG = -1e30
TILE = 256


def attend_kernel(*refs, chunks, sources, opening, closing):
    refs = list(refs)
    limit_ref, me_ref = refs.pop(0), refs.pop(0)
    q_near, q_rest = refs.pop(0), refs.pop(0)
    q_refs = [r.at[i] for r in (q_near, q_rest) for i in range(GROUP // 2)]
    kv_refs = [refs.pop(0) for _ in range(sources)]
    old = None if opening else [refs.pop(0) for _ in range(2)]
    o_ref = refs.pop(0) if closing else None
    m_ref, a_ref = refs.pop(0), refs.pop(0)
    qs, ks, vs, s0, s1, x0, x1 = refs
    units, rows, _ = qs.shape
    span = ks.shape[1]
    frames = span // GROUP
    half = frames // 2
    whole = GROUP
    at_k = frames + half
    limit, me = limit_ref[0], me_ref[0]
    spans = 4

    low = low_lanes(frames)
    for j in range(GROUP):
        q = q_refs[j][0:frames, :]
        qs[j, 0:frames, :] = jnp.where(low, q, jnp.zeros_like(q))
        qs[j, frames:rows, :] = jnp.where(low, jnp.zeros_like(q), q)
    for u in range(whole, units):
        for k in range(rows // half):
            qs[u, k * half : (k + 1) * half, :] = q_refs[(u - whole) * (rows // half) + k][frames:at_k, :]
    ones = jnp.ones((span, LANES), jnp.bfloat16)

    def scores(u, t):
        team = jnp.where(u < whole, 0, 1)
        return lax.dot_general(
            qs[u], ks[team, t * TILE : (t + 1) * TILE, :], (((1,), (1,)), ((), ())), preferred_element_type=jnp.float32
        )

    def lane_max(s):
        return jnp.maximum(s[:, :LANES], s[:, LANES:])

    def spread_max(top):
        return jnp.broadcast_to(jnp.max(top, axis=1, keepdims=True), top.shape)

    def begin(u, s_out, x_out):
        top = None
        for t in range(span // TILE):
            s = scores(u, t)
            s_out[:, t * TILE : (t + 1) * TILE] = s
            top = lane_max(s) if top is None else jnp.maximum(top, lane_max(s))
        x_out[...] = spread_max(top)

    def both(u, s_in, x_in, nxt, s_out, x_out, fresh, was):
        team = jnp.where(u < whole, 0, 1)
        if fresh:
            m_new = x_in[...]
        else:
            m_old = was[0][u]
            m_new = jnp.maximum(m_old, x_in[...])
        m_two = jnp.concatenate([m_new, m_new], axis=1)
        m_ref[u] = m_new
        total, top = None, None
        for t in range(span // TILE):
            at = slice(t * TILE, (t + 1) * TILE)
            p = jnp.exp2(s_in[:, at] - m_two).astype(jnp.bfloat16)
            s = scores(nxt, t)
            s_out[:, at] = s
            top = lane_max(s) if top is None else jnp.maximum(top, lane_max(s))
            term = jnp.dot(p, vs[team, at, :], preferred_element_type=jnp.float32)
            total = term if total is None else total + term
        x_out[...] = spread_max(top)
        if fresh:
            a_ref[u] = total
        else:
            keep = jnp.exp2(m_old - m_new)
            a_ref[u] = was[1][u] * jnp.concatenate([keep, keep], axis=1) + total

    for c, blocks in enumerate(chunks):
        fresh = opening and c == 0
        was = old if c == 0 else (m_ref, a_ref)
        starts = [
            lax.rem(me // GROUP + spans - up, spans) * span + member(me, hop, -1) * frames for _, _, hop, up in blocks
        ]
        lowest, at_low, highest = starts[0], 0, starts[0]
        for i, start in enumerate(starts[1:], 1):
            at_low = jnp.where(start < lowest, i * frames, at_low)
            lowest = jnp.minimum(lowest, start)
            highest = jnp.maximum(highest, start)

        @pl.when(limit > lowest)
        def _():
            for i, (source, index, _, _) in enumerate(blocks):
                at = slice(i * frames, (i + 1) * frames)
                kv = kv_refs[source]
                part = lambda n: kv[index, n * frames : (n + 1) * frames, :]
                ks[0, at, :] = part(0)
                ks[1, at, :] = part(2)
                vs[0, at, :LANES] = part(1)
                vs[1, at, :LANES] = part(2)
            vs[0, :, LANES:] = ones
            vs[1, :, LANES:] = ones

            @pl.when(limit < highest + frames)
            def _():
                row = lax.broadcasted_iota(jnp.int32, (frames, LANES), 0)
                for team in range(2):
                    spare = ks[team, pl.ds(pl.multiple_of(at_low, frames), 16), :].astype(jnp.float32)[0:1]
                    for i, start in enumerate(starts):
                        at = slice(i * frames, (i + 1) * frames)
                        alive = row < limit - start
                        k = ks[team, at, :].astype(jnp.float32)
                        ks[team, at, :] = jnp.where(alive, k, spare).astype(jnp.bfloat16)
                        for side in range(2):
                            lanes = slice(side * LANES, (side + 1) * LANES)
                            v = vs[team, at, lanes].astype(jnp.float32)
                            vs[team, at, lanes] = jnp.where(alive, v, 0.0).astype(jnp.bfloat16)

            begin(0, s0, x0)

            def step(i, carry):
                both(2 * i, s0, x0, 2 * i + 1, s1, x1, fresh, was)
                both(2 * i + 1, s1, x1, jnp.minimum(2 * i + 2, units - 1), s0, x0, fresh, was)
                return carry

            lax.fori_loop(0, units // 2, step, 0)

        if c == 0:

            @pl.when(limit <= lowest)
            def _():
                if fresh:
                    m_ref[...] = jnp.full(m_ref.shape, NEG, jnp.float32)
                    a_ref[...] = jnp.zeros(a_ref.shape, jnp.float32)
                else:
                    m_ref[...] = was[0][...]
                    a_ref[...] = was[1][...]

    if closing:
        for u in range(units):
            o = a_ref[u, :, :LANES] / a_ref[u, :, LANES:]
            if u < whole:
                o_ref[member(me, u, -1), 0:frames, :] = jnp.where(low, o[:frames], o[frames:]).astype(jnp.bfloat16)
            else:
                o = jnp.where(low_lanes(rows), 0.0, o).astype(jnp.bfloat16)
                for k in range(rows // half):
                    place = member(me, (u - whole) * (rows // half) + k, -1)
                    o_ref[place, frames:at_k, :] = o[k * half : (k + 1) * half]


def output_kernel(o_ref, w_ref, bias_ref, stem_ref, attended_ref, encoded_ref):
    frames, _ = stem_ref.shape
    half = frames // 2
    total = None
    for g in range(GROUP):
        at = ab_start(g)
        term = jnp.dot(o_ref[g, 0:frames, :], w_ref[at : at + LANES, :], preferred_element_type=jnp.float32)
        total = term if total is None else total + term
        if g % 2:
            at = s_start(g) - 64
            shared = jnp.concatenate(
                [o_ref[g - 1, frames : frames + half, :], o_ref[g, frames : frames + half, :]], axis=0
            )
            total = total + jnp.dot(shared, w_ref[at : at + LANES, :], preferred_element_type=jnp.float32)
    total = total + bias_ref[...]
    attended_ref[...] = total.astype(jnp.bfloat16)
    encoded_ref[...] = (stem_ref[...].astype(jnp.float32) + total).astype(jnp.bfloat16)


STEM_MIB = 58
W2_PARTS = 6
VMEM = pltpu.MemorySpace.VMEM
SMEM = pltpu.MemorySpace.SMEM


def spec(space):
    return pl.BlockSpec(memory_space=space)


def params(mib):
    return pltpu.CompilerParams(vmem_limit_bytes=mib * 2**20)


def shards(
    spectrum, valid_frames, inlet_weight, inlet_bias, stride_weight, stride_bias, norm_gain, norm_bias,
    projection_weight, query_value_bias, out_weight, out_bias,
):
    mel_rows, channels = spectrum.shape
    frames = mel_rows // 2
    width = projection_weight.shape[0]
    count = lax.axis_size("seq")
    me = lax.axis_index("seq")
    down = [(i, i + 1) for i in range(count - 1)]
    up = [(i + 1, i) for i in range(count - 1)]
    early = lax.ppermute(spectrum[mel_rows - 2 :], "seq", down)
    late = lax.ppermute(spectrum[:2], "seq", up)
    here = me.astype(jnp.int32).reshape(1)
    row = lambda v: v.reshape(1, width)
    bf16 = lambda *dims: jax.ShapeDtypeStruct(dims, jnp.bfloat16)
    f32 = lambda *dims: jax.ShapeDtypeStruct(dims, jnp.float32)

    *messages, stem = pl.pallas_call(
        stem_kernel,
        name="stem",
        out_shape=(bf16(4 * frames + frames // 2, LANES),) * GROUP + (bf16(frames, width),),
        in_specs=[spec(SMEM)] + [spec(VMEM)] * 8 + [spec(pltpu.MemorySpace.HBM)] * 3,
        out_specs=(spec(VMEM),) * (GROUP + 1),
        scratch_shapes=[
            pltpu.VMEM((3 * channels, width), jnp.bfloat16),
            pltpu.VMEM((3 * width, width), jnp.bfloat16),
            pltpu.VMEM((width, 3 * width), jnp.bfloat16),
            pltpu.VMEM((frames + 8, width), jnp.float32),
            pltpu.VMEM((mel_rows, channels), jnp.float32),
            pltpu.VMEM((frames + 8, 2 * channels), jnp.float32),
            pltpu.VMEM((GROUP, 4 * frames + frames // 2, LANES), jnp.bfloat16),
            pltpu.SemaphoreType.DMA((4 + W2_PARTS,)),
        ],
        compiler_params=params(STEM_MIB),
        cost_estimate=pl.CostEstimate(flops=4 * 10**9, bytes_accessed=20 * 10**6, transcendentals=0),
    )(
        here, early, late, spectrum, inlet_bias, stride_bias, norm_gain, norm_bias, query_value_bias,
        inlet_weight.reshape(3 * channels, width), stride_weight.reshape(3 * width, width), projection_weight,
    )

    spans = count // GROUP

    def send(v, r):
        dz, dx = HOPS[r]
        there = lambda i: i // 8 * 8 + (i // 4 + dz) % 2 * 4 + (i + dx) % 4
        return lax.ppermute(v, "seq", [(i, there(i)) for i in range(count)])

    def shift(v, by):
        return lax.ppermute(v, "seq", [(i, (i + by * GROUP) % count) for i in range(count)])

    def pack(parts, after):
        return pl.pallas_call(
            pack_kernel,
            name="pack",
            out_shape=(bf16(len(parts), 3 * frames, LANES), bf16(len(parts), frames + frames // 2, LANES)),
            in_specs=[spec(VMEM)] * len(parts) + [spec(pl.ANY)] * len(after),
            out_specs=(spec(VMEM),) * 2,
            compiler_params=params(4),
            cost_estimate=pl.CostEstimate(flops=10**8, bytes_accessed=10**6, transcendentals=0),
        )(*parts, *after)

    blocks = [messages[0]] + [send(messages[r], r) for r in range(1, GROUP)]
    cut = GROUP // 2
    near, query_near = pack(blocks[:cut], [])
    below_near = shift(near, 1)
    above_near = shift(near, spans - 1)
    rest, query_rest = pack(blocks[cut:], [near])
    below_rest = shift(rest, 1)
    above_rest = shift(rest, spans - 1)
    far_near = shift(below_near, 1)
    far_rest = shift(above_rest, spans - 1)

    span = GROUP * frames
    rows = 2 * frames
    units = GROUP + GROUP // 4
    scratch = [
        pltpu.VMEM((units, rows, LANES), jnp.bfloat16),
        pltpu.VMEM((2, span, LANES), jnp.bfloat16),
        pltpu.VMEM((2, span, 2 * LANES), jnp.bfloat16),
        pltpu.VMEM((rows, span), jnp.float32),
        pltpu.VMEM((rows, span), jnp.float32),
        pltpu.VMEM((rows, LANES), jnp.float32),
        pltpu.VMEM((rows, LANES), jnp.float32),
    ]
    shapes = ((units, rows, LANES), (units, rows, 2 * LANES))

    def attend(chunks, arrays, state, closing):
        operands = [valid_frames, here, query_near, query_rest, *arrays, *(state or ())]
        out = (bf16(GROUP, frames + frames // 2, LANES),) if closing else tuple(f32(*s) for s in shapes)
        body = lambda *refs: attend_kernel(
            *refs, chunks=chunks, sources=len(arrays), opening=state is None, closing=closing
        )
        extra = [pltpu.VMEM(s, jnp.float32) for s in shapes] if closing else []
        return pl.pallas_call(
            body,
            out_shape=out,
            in_specs=[spec(SMEM)] * 2 + [spec(VMEM)] * (len(operands) - 2),
            out_specs=tuple(spec(VMEM) for _ in out),
            scratch_shapes=extra + scratch,
            compiler_params=params(30),
            cost_estimate=pl.CostEstimate(flops=4 * 10**9 * len(chunks), bytes_accessed=5 * 10**6, transcendentals=0),
        )(*operands)

    lows, highs = range(cut), range(cut, GROUP)
    mine = [(0, r, r, 0) for r in lows] + [(1, r - cut, r, 0) for r in highs]
    first = [(0, r, r, 1) for r in lows] + [(1, r, r, spans - 1) for r in lows]
    second = [(0, r - cut, r, 1) for r in highs] + [(1, r - cut, r, spans - 1) for r in highs]
    third = [(0, r, r, 2) for r in lows] + [(1, r - cut, r, 2) for r in highs]
    state = attend([mine], [near, rest], None, False)
    state = attend([first], [below_near, above_near], state, False)
    state = attend([second], [below_rest, above_rest], state, False)
    (mixed,) = attend([third], [far_near, far_rest], state, True)
    teams = [list(range(i, i + GROUP)) for i in range(0, count, GROUP)]
    mixed = lax.all_to_all(mixed, "seq", 0, 0, axis_index_groups=teams)
    attended, encoded = pl.pallas_call(
        output_kernel,
        name="output",
        out_shape=(bf16(frames, width),) * 2,
        in_specs=[spec(VMEM)] * 4,
        out_specs=(spec(VMEM),) * 2,
        compiler_params=params(20),
        cost_estimate=pl.CostEstimate(flops=10**9, bytes_accessed=4 * 10**6, transcendentals=0),
    )(mixed, out_weight, row(out_bias), stem)
    return attended, encoded


def solution(mesh):
    in_specs = (P(("dp", "seq"), None), P("dp"), P(), P(), P(), P(), P(), P(), P(), P(), P(), P())
    out_specs = (P(("dp", "seq"), None), P(("dp", "seq"), None))

    return jax.shard_map(shards, mesh=mesh, in_specs=in_specs, out_specs=out_specs, check_vma=False)
```
